256 devices in a mesh: grp: 16 (over x, y_hi, core), rng: 16 (over z, y_lo).
Axes of the slice: x: 4, y: 4 (y_hi: 2, y_lo: 2; y = y_hi * 2 + y_lo), z: 8, core: 2. Of those that a mesh axis runs over, the one named last changes fastest.
Arguments:
- features: bfloat16 [65536, 1024], P(('grp', 'rng')), may hold values from -6 to 6
- query_weight: bfloat16 [1024, 1024], replicated
- key_weight: bfloat16 [1024, 1024], replicated
- value_weight: bfloat16 [1024, 1024], replicated, may hold values from -0.1875 to 0.1875
- out_weight: bfloat16 [1024, 1024], replicated, may hold values from -0.1875 to 0.1875
- band_reach: int32 [256], P(('grp', 'rng')), may hold values from 16 to 128, as said below
- long_peers: int32 [512, 6], P(('grp', 'rng')), may hold values from 0 to 15, as said below
- long_count: int32 [512], P(('grp', 'rng')), may hold values from 0 to 6, as said below
- send_tile: int32 [256, 16], P(('grp', 'rng')), may hold values from 0 to 3
Outputs:
- updated: bfloat16 [65536, 1024], P(('grp', 'rng'))
The draws below stay inside these ranges and needn't reach their ends.
Inputs may be any that keep to these rules, and one draw needn't show every extreme that they name: `band_reach`: some range has 128 in every draw. `long_peers`: the 6 entries of a query tile in region g are distinct regions other than g; only the first long_count entries are used. `long_count`: some query tile has 6 in every draw.
All inputs are finite; a program needn't handle non-finite values.
Results may differ from the reference program's by a relative error of at most 0.0064.
Values may be sent and summed in bfloat16 or wider, within the bound.
A program may use at most 128 MiB of HBM per device.

```python
import jax
import jax.numpy as jnp
from jax import lax

D = 1024
HEADS = 16
TOK_DEV = 256
TILE = 128
PORTAL = 64
MAXLONG = 6
REGION = 4096
NODES = 65536
QTILES = 512
N_GRP = 16
N_RNG = 16


def projection_pair(key):
    key_part = jax.random.normal(jax.random.fold_in(key, 12), (D, D), jnp.float32) * D ** (-0.5)
    query_noise = jax.random.normal(jax.random.fold_in(key, 11), (D, D), jnp.float32)
    query_part = query_noise * (D // 8) ** (-0.5)
    return (query_part, key_part)


def draw_query_weight(key, part):
    return projection_pair(key)[0].astype(jnp.bfloat16)


def draw_key_weight(key, part):
    return projection_pair(key)[1].astype(jnp.bfloat16)


def draw_band_reach(key, part):
    device_total = NODES // TOK_DEV
    reaches = jax.random.randint(jax.random.fold_in(key, 21), (device_total,), TILE // 8, TILE + 1)
    chosen = jax.random.randint(jax.random.fold_in(key, 22), (), 0, device_total)
    return jnp.where(jnp.arange(device_total) == chosen, TILE, reaches).astype(jnp.int32)


def draw_long_count(key, part):
    device_total = NODES // TOK_DEV
    per_device = TOK_DEV // TILE
    heavy_ranges = jax.random.randint(jax.random.fold_in(key, 31), (device_total,), 0, 4) == 0
    chosen = jax.random.randint(jax.random.fold_in(key, 32), (), 0, device_total)
    heavy_ranges = heavy_ranges | (jnp.arange(device_total) == chosen)
    device_cap = jnp.where(heavy_ranges, MAXLONG, MAXLONG // 3)
    tile_cap = jnp.repeat(device_cap, per_device)
    counts = jax.random.randint(jax.random.fold_in(key, 33), (QTILES,), 0, 1 << 20) % (tile_cap + 1)
    counts = jnp.where(jnp.arange(QTILES) == chosen * per_device, MAXLONG, counts)
    return counts.astype(jnp.int32)


def draw_long_peers(key, part):
    regions = NODES // REGION
    ranking_keys = jax.random.randint(jax.random.fold_in(key, 41), (QTILES, regions - 1), 0, 1 << 20) * regions
    ranking_keys = ranking_keys + jnp.arange(regions - 1, dtype=jnp.int32)[None, :]
    ranking = jnp.argsort(ranking_keys, axis=1, stable=True)[:, :MAXLONG].astype(jnp.int32)
    home_region = jnp.arange(QTILES, dtype=jnp.int32) * TILE // REGION
    return jnp.where(ranking >= home_region[:, None], ranking + 1, ranking).astype(jnp.int32)


def touch_ends(result, stream_key, least, top_value):
    spot = [jax.random.randint(jax.random.fold_in(stream_key, axis), (), 0, length) for axis, length in enumerate(result.shape)]
    main_axis = result.shape.index(max(result.shape))
    next_to = spot[:main_axis] + [(spot[main_axis] + 1) % result.shape[main_axis]] + spot[main_axis + 1:]
    return result.at[tuple(spot)].set(least).at[tuple(next_to)].set(top_value)


def block_levels(key, extent, shards, smallest, high):
    def one(dim, shards_of):
        draws = jax.random.uniform(jax.random.fold_in(jax.random.fold_in(key, 6), dim), (shards_of,), jnp.float32, smallest / len(shards), high / len(shards))
        return jnp.repeat(jnp.exp(draws), extent[dim] // shards_of).reshape((-1,) + (1,) * (len(extent) - dim - 1))

    level = one(*shards[0])
    for cut in shards[1:]:
        level = level * one(*cut)
    return level


def bell_draw(rng, dims, spread, reach, cuts=(), held_as=jnp.bfloat16):
    values = jax.random.normal(rng, dims, jnp.float32) * spread
    if len(cuts) > 0:
        values = block_levels(rng, dims, cuts, -0.22, 0.18) * values
    return jnp.clip(values, min=-reach, max=reach).astype(held_as)


def setup_inputs(seed: int = 0) -> dict:
    streams_of = jax.random.split(jax.random.key(seed), 10)
    features = bell_draw(streams_of[0], (NODES, D), 1.0, 6.0, ((0, 256),))
    query_weight = draw_query_weight(jax.random.fold_in(streams_of[9], 71), 0)
    key_weight = draw_key_weight(jax.random.fold_in(streams_of[9], 71), 0)
    value_weight = bell_draw(streams_of[3], (D, D), D ** -0.5, 0.1875)
    out_weight = bell_draw(streams_of[4], (D, D), D ** -0.5, 0.1875)
    band_reach = draw_band_reach(jax.random.fold_in(streams_of[9], 71), 0)
    long_peers = draw_long_peers(jax.random.fold_in(streams_of[9], 71), 0)
    long_count = draw_long_count(jax.random.fold_in(streams_of[9], 71), 0)
    send_tile = touch_ends(jax.random.randint(streams_of[8], (N_GRP * N_RNG, N_GRP), 0, TOK_DEV // PORTAL), jax.random.fold_in(streams_of[8], 1), 0, (TOK_DEV // PORTAL) - 1).astype(jnp.int32)
    return {"features": features, "query_weight": query_weight, "key_weight": key_weight, "value_weight": value_weight, "out_weight": out_weight, "band_reach": band_reach, "long_peers": long_peers, "long_count": long_count, "send_tile": send_tile}


EPSILON = 1e-06

def reference(features, query_weight, key_weight, value_weight, out_weight, band_reach, long_peers, long_count, send_tile):
    head_dim = D // HEADS
    score_scale = head_dim ** (-0.5)
    widened = features.astype(jnp.float32)
    normed = (widened * lax.rsqrt(lax.optimization_barrier(jnp.mean(widened * widened, axis=1, keepdims=True)) + EPSILON)).astype(jnp.bfloat16)
    queries = jnp.dot(normed, query_weight, preferred_element_type=jnp.float32).astype(jnp.bfloat16)
    keys_all = jnp.dot(normed, key_weight, preferred_element_type=jnp.float32).astype(jnp.bfloat16)
    values_all = jnp.dot(normed, value_weight, preferred_element_type=jnp.float32).astype(jnp.bfloat16)
    offsets = jnp.arange(3 * TILE, dtype=jnp.int32) - TILE
    places = jnp.arange(TILE, dtype=jnp.int32)
    inside_gap = jnp.abs(places[:, None] - offsets[None, :])
    portal_span = jnp.arange(PORTAL, dtype=jnp.int32)
    slot_ids = jnp.arange(MAXLONG, dtype=jnp.int32)

    def one_tile(tile_num):
        row_start = tile_num * TILE
        device_num = row_start // TOK_DEV
        group_num = device_num // N_RNG
        rank_num = device_num % N_RNG
        position = row_start - group_num * REGION
        band_rows = group_num * REGION + (position + offsets) % REGION
        sources = long_peers[tile_num] * N_RNG + rank_num
        portal_num = send_tile[sources, group_num]
        long_rows = (sources * TOK_DEV + portal_num * PORTAL)[:, None] + portal_span[None, :]
        key_rows = jnp.concatenate([band_rows.astype(jnp.int32), long_rows.reshape(-1).astype(jnp.int32)])
        query_blk = lax.dynamic_slice_in_dim(queries, row_start.astype(jnp.int32), TILE, 0)
        query_blk = query_blk.astype(jnp.float32).reshape(TILE, HEADS, head_dim)
        key_blk = jnp.take(keys_all, key_rows, axis=0).astype(jnp.float32).reshape(-1, HEADS, head_dim)
        value_blk = jnp.take(values_all, key_rows, axis=0).astype(jnp.float32).reshape(-1, HEADS, head_dim)
        scores = jnp.einsum('qhd,khd->hqk', query_blk, key_blk) * score_scale
        band_ok = inside_gap <= band_reach[device_num]
        long_ok = jnp.repeat(slot_ids < long_count[tile_num], PORTAL)
        allowed = jnp.concatenate([band_ok, jnp.broadcast_to(long_ok[None, :], (TILE, MAXLONG * PORTAL))], axis=1)
        scores = jnp.where(allowed[None], scores, -jnp.inf)
        highest = lax.optimization_barrier(jnp.max(scores, axis=2, keepdims=True))
        weights = jnp.exp(scores - highest)
        probabilities = (weights / lax.optimization_barrier(jnp.sum(weights, axis=2, keepdims=True))).astype(jnp.bfloat16)
        mixed = jnp.einsum('hqk,khd->qhd', probabilities.astype(jnp.float32), value_blk)
        return mixed.reshape(TILE, D).astype(jnp.bfloat16)
    attended = lax.map(one_tile, jnp.arange(QTILES, dtype=jnp.int32)).reshape(NODES, D)
    projected = jnp.dot(attended, out_weight, preferred_element_type=jnp.float32)
    return (widened + projected).astype(jnp.bfloat16)
```

```python
import functools

import jax
import jax.numpy as jnp
from jax import lax
from jax.experimental import pallas as pl
from jax.experimental.pallas import tpu as pltpu
from jax.sharding import PartitionSpec as P

MESH = pl.DeviceIdType.MESH
F32 = jnp.float32
BF16 = jnp.bfloat16

EPSILON = 1e-06
D = 1024
ROWS = 256
TILE = 128
PORTAL = 64
MAXLONG = 6
LANES = 128
PAIRS = D // LANES
SCALE = 64 ** (-0.5)
FLOOR = -3.0e38

GRAY = {0: 0, 1: 1, 2: 3, 3: 2}
X_ORDER = ((1, 0), (3, 0), (1, 1), (3, 1), (2, 0), (2, 1))
NEAR_BLOCKS = 2 * ROWS // PORTAL


def project(src, block, count, weight, dst, dst_block, scale=None):
    @pl.loop(0, D // 256)
    def _(step):
        columns = pl.ds(pl.multiple_of(step * 256, 256), 256)
        total = jnp.dot(
            src[pl.ds(block, count)].reshape(count * PORTAL, D),
            weight[:, columns],
            preferred_element_type=F32,
        ).astype(BF16)
        if scale is not None:
            total = total * jnp.asarray(scale, BF16)
        dst[pl.ds(dst_block, count), :, columns] = total.reshape(count, PORTAL, 256)


def kernel(
    reach_ref,
    peers_ref,
    count_ref,
    pick_ref,
    feat_hbm,
    wq_hbm,
    wk_hbm,
    wv_hbm,
    wo_hbm,
    out_ref,
    feat,
    wq,
    wk,
    wv,
    wo,
    normed,
    partner,
    partner_pick,
    halo,
    arrived,
    stage_own,
    stage_far,
    queries,
    keys,
    values,
    attended,
    bias_near,
    bias_far,
    acc_near,
    sum_near,
    max_near,
    in_sem,
    send_own,
    recv_own,
    send_far,
    recv_far,
    send_y,
    recv_y,
    send_halo,
    recv_halo,
):
    g = lax.axis_index("grp")
    r = lax.axis_index("rng")
    x, row_bit, core = g // 4, (g // 2) % 2, g % 2

    def device(dx, dy, dc):
        return (
            lax.rem(x + dx, 4) * 4 + lax.rem(row_bit + dy, 2) * 2 + lax.rem(core + dc, 2),
            r,
        )

    above = (g, lax.rem(r + 1, 16))
    below = (g, lax.rem(r + 15, 16))
    row_flows = X_ORDER + ((0, 1),)

    loads = [
        pltpu.make_async_copy(src, dst, in_sem.at[i])
        for i, (src, dst) in enumerate(
            ((feat_hbm, feat), (wq_hbm, wq), (wk_hbm, wk), (wv_hbm, wv), (wo_hbm, wo))
        )
    ]
    for load in loads:
        load.start()

    barrier = pltpu.get_barrier_semaphore()
    friends = [device(dx, 0, dc) for dx, dc in row_flows] + [device(0, 1, 0), above, below]
    for friend in friends:
        pl.semaphore_signal(barrier, inc=1, device_id=friend, device_id_type=MESH)

    loads[0].wait()

    @pl.loop(0, ROWS // PORTAL)
    def _(block):
        rows = pl.ds(pl.multiple_of(block * PORTAL, PORTAL), PORTAL)
        widened = feat[rows, :].astype(F32)
        factor = lax.rsqrt(jnp.mean(widened * widened, axis=1, keepdims=True) + EPSILON)
        normed[block] = (widened * factor).astype(BF16)

    def pick_own(flow):
        dx, dc = row_flows[flow]
        target, _ = device(dx, 0, dc)
        stage_own[flow] = normed[pick_ref[0, target]]

    def slot_of_flow(dx, dc, far):
        return 8 * far + 2 * GRAY[dx] + dc

    for flow in range(len(row_flows)):
        pick_own(flow)

    pl.semaphore_wait(barrier, len(friends))

    cross = [
        pltpu.make_async_remote_copy(
            src_ref=normed, dst_ref=partner, send_sem=send_y.at[0], recv_sem=recv_y.at[0],
            device_id=device(0, 1, 0), device_id_type=MESH,
        ),
        pltpu.make_async_remote_copy(
            src_ref=pick_ref, dst_ref=partner_pick, send_sem=send_y.at[1], recv_sem=recv_y.at[1],
            device_id=device(0, 1, 0), device_id_type=MESH,
        ),
    ]
    for copy in cross:
        copy.start()
    own = []
    for flow, (dx, dc) in enumerate(row_flows):
        copy = pltpu.make_async_remote_copy(
            src_ref=stage_own.at[flow],
            dst_ref=arrived.at[slot_of_flow(dx, dc, 0)],
            send_sem=send_own.at[flow],
            recv_sem=recv_own.at[flow],
            device_id=device(dx, 0, dc),
            device_id_type=MESH,
        )
        copy.start()
        own.append(copy)

    reach = reach_ref[0]
    place_q = lax.broadcasted_iota(jnp.int32, (ROWS, ROWS), 0)
    place_k = lax.broadcasted_iota(jnp.int32, (ROWS, ROWS), 1)
    bias_near[...] = jnp.where(jnp.abs(place_q - place_k) <= reach, 0.0, -jnp.inf)
    tile_q = lax.broadcasted_iota(jnp.int32, (TILE, TILE), 0)
    tile_k = lax.broadcasted_iota(jnp.int32, (TILE, TILE), 1)
    slot_of = lax.broadcasted_iota(jnp.int32, (TILE, MAXLONG * PORTAL), 1) // PORTAL
    for tile in range(2):
        gap = (tile_q - tile_k if tile == 0 else tile_k - tile_q) + TILE
        bias_far[tile, :, :TILE] = jnp.where(gap <= reach, 0.0, -jnp.inf)
        bias_far[tile, :, TILE:] = jnp.where(slot_of < count_ref[tile], 0.0, -jnp.inf)

    loads[1].wait()
    project(normed, 0, 4, wq, queries, 0, SCALE)
    loads[2].wait()
    project(normed, 0, 4, wk, keys, 2)
    loads[3].wait()
    project(normed, 0, 4, wv, values, 2)

    even = lax.broadcasted_iota(jnp.int32, (TILE, LANES), 1) < LANES // 2

    def attend(tile, lanes, key_rows, value_rows, bias):
        query = queries[pl.ds(tile * 2, 2), :, lanes].reshape(TILE, LANES)
        none = jnp.zeros_like(query)
        both = jnp.concatenate(
            [jnp.where(even, query, none), jnp.where(even, none, query)], axis=0
        )
        scores = lax.dot_general(
            both, key_rows, (((1,), (1,)), ((), ())), preferred_element_type=F32
        )
        scores = scores + jnp.concatenate([bias, bias], axis=0)
        highest = jnp.maximum(jnp.max(scores, axis=1, keepdims=True), FLOOR)
        weights = jnp.exp(scores - highest).astype(BF16)
        wide = jnp.concatenate([value_rows, jnp.ones_like(value_rows)], axis=1)
        mixed = jnp.dot(weights, wide, preferred_element_type=F32)
        top = jnp.broadcast_to(highest, (2 * TILE, LANES))
        return (
            jnp.where(even, mixed[:TILE, :LANES], mixed[TILE:, :LANES]),
            jnp.where(even, mixed[:TILE, LANES:], mixed[TILE:, LANES:]),
            jnp.where(even, top[:TILE], top[TILE:]),
        )

    @pl.loop(0, PAIRS)
    def _(pair):
        lanes = pl.ds(pl.multiple_of(pair * LANES, LANES), LANES)
        near = pl.ds(2, 4)
        key_rows = keys[near, :, lanes].reshape(ROWS, LANES)
        value_rows = values[near, :, lanes].reshape(ROWS, LANES)
        for tile in range(2):
            rows = pl.ds(tile * TILE, TILE)
            mixed, total, top = attend(
                tile, lanes, key_rows, value_rows, bias_near[rows, :]
            )
            acc_near[rows, lanes] = mixed
            sum_near[rows, lanes] = total
            max_near[rows, lanes] = top

    for copy in own:
        copy.wait_recv()

    def project_slots(first, count):
        project(arrived, first, count, wk, keys, NEAR_BLOCKS + first)
        project(arrived, first, count, wv, values, NEAR_BLOCKS + first)

    project_slots(1, 7)

    for copy in cross:
        copy.wait()

    def far_rows(target):
        return partner[partner_pick[0, target]]

    far = []
    for flow, (dx, dc) in enumerate(row_flows):
        target, _ = device(dx, 0, dc)
        stage_far[flow] = far_rows(target)
    for flow, (dx, dc) in enumerate(row_flows):
        copy = pltpu.make_async_remote_copy(
            src_ref=stage_far.at[flow],
            dst_ref=arrived.at[slot_of_flow(dx, dc, 1)],
            send_sem=send_far.at[flow],
            recv_sem=recv_far.at[flow],
            device_id=device(dx, 0, dc),
            device_id_type=MESH,
        )
        copy.start()
        far.append(copy)
    edges = [
        pltpu.make_async_remote_copy(
            src_ref=normed.at[pl.ds(2, 2)], dst_ref=halo.at[pl.ds(0, 2)],
            send_sem=send_halo.at[0], recv_sem=recv_halo.at[0],
            device_id=above, device_id_type=MESH,
        ),
        pltpu.make_async_remote_copy(
            src_ref=normed.at[pl.ds(0, 2)], dst_ref=halo.at[pl.ds(2, 2)],
            send_sem=send_halo.at[1], recv_sem=recv_halo.at[1],
            device_id=below, device_id_type=MESH,
        ),
    ]
    for copy in edges:
        copy.start()
    arrived[8] = far_rows(g)

    for flow in (6, 0, 1, 2, 3):
        far[flow].wait_recv()
    project_slots(8, 6)
    for copy in edges:
        copy.wait_recv()
    for weight, dst in ((wk, keys), (wv, values)):
        project(halo, 0, 2, weight, dst, 0)
        project(halo, 2, 2, weight, dst, 6)
    for flow in (4, 5):
        far[flow].wait_recv()
    project_slots(14, 2)

    def slot_start(tile, entry):
        peer = peers_ref[tile, entry]
        dx = lax.rem(x + 4 - lax.div(peer, 4), 4)
        place = dx + lax.div(dx, 2) * (1 - 2 * lax.rem(dx, 2))
        other = lax.rem(lax.div(peer, 2) + row_bit, 2)
        turn = lax.rem(peer + core, 2)
        return NEAR_BLOCKS + 8 * other + 2 * place + turn

    for tile in range(2):
        rows = pl.ds(tile * TILE, TILE)
        edge = pl.ds(6 * tile, 2)
        starts = [slot_start(tile, entry) for entry in range(MAXLONG)]

        @pl.loop(0, PAIRS)
        def _(pair):
            lanes = pl.ds(pl.multiple_of(pair * LANES, LANES), LANES)

            def gathered(ref):
                return jnp.concatenate(
                    [ref[edge, :, lanes].reshape(TILE, LANES)]
                    + [ref[start, :, lanes] for start in starts],
                    axis=0,
                )

            mixed, total, top = attend(
                tile, lanes, gathered(keys), gathered(values), bias_far[tile]
            )
            near_top = max_near[rows, lanes]
            highest = jnp.maximum(near_top, top)
            near_part = jnp.exp(near_top - highest)
            far_part = jnp.exp(top - highest)
            mixed = acc_near[rows, lanes] * near_part + mixed * far_part
            total = sum_near[rows, lanes] * near_part + total * far_part
            attended[rows, lanes] = (mixed / total).astype(BF16)

    loads[4].wait()

    @pl.loop(0, D // 256)
    def _(step):
        columns = pl.ds(pl.multiple_of(step * 256, 256), 256)
        total = jnp.dot(attended[...], wo[:, columns], preferred_element_type=F32)
        out_ref[:, columns] = (feat[:, columns].astype(F32) + total).astype(BF16)

    for copy in own + far + edges:
        copy.wait_send()


def local(
    features,
    query_weight,
    key_weight,
    value_weight,
    out_weight,
    band_reach,
    long_peers,
    long_count,
    send_tile,
):
    smem = pl.BlockSpec(memory_space=pltpu.SMEM)
    hbm = pl.BlockSpec(memory_space=pl.ANY)
    flows = len(X_ORDER) + 1
    dma = pltpu.SemaphoreType.DMA
    return pl.pallas_call(
        kernel,
        name="layer",
        out_shape=jax.ShapeDtypeStruct((ROWS, D), BF16),
        in_specs=[smem] * 4 + [hbm] * 5,
        out_specs=pl.BlockSpec(memory_space=pltpu.VMEM),
        scratch_shapes=[
            pltpu.VMEM((ROWS, D), BF16),
            pltpu.VMEM((D, D), BF16),
            pltpu.VMEM((D, D), BF16),
            pltpu.VMEM((D, D), BF16),
            pltpu.VMEM((D, D), BF16),
            pltpu.VMEM((4, PORTAL, D), BF16),
            pltpu.VMEM((4, PORTAL, D), BF16),
            pltpu.SMEM((1, 16), jnp.int32),
            pltpu.VMEM((4, PORTAL, D), BF16),
            pltpu.VMEM((16, PORTAL, D), BF16),
            pltpu.VMEM((flows, PORTAL, D), BF16),
            pltpu.VMEM((flows, PORTAL, D), BF16),
            pltpu.VMEM((4, PORTAL, D), BF16),
            pltpu.VMEM((NEAR_BLOCKS + 16, PORTAL, D), BF16),
            pltpu.VMEM((NEAR_BLOCKS + 16, PORTAL, D), BF16),
            pltpu.VMEM((ROWS, D), BF16),
            pltpu.VMEM((ROWS, ROWS), F32),
            pltpu.VMEM((2, TILE, TILE + MAXLONG * PORTAL), F32),
            pltpu.VMEM((ROWS, D), F32),
            pltpu.VMEM((ROWS, D), F32),
            pltpu.VMEM((ROWS, D), F32),
            dma((5,)),
            dma((flows,)),
            dma((flows,)),
            dma((flows,)),
            dma((flows,)),
            dma((2,)),
            dma((2,)),
            dma((2,)),
            dma((2,)),
        ],
        compiler_params=pltpu.CompilerParams(
            collective_id=0, has_side_effects=True, vmem_limit_bytes=60 * 1024 * 1024
        ),
    )(
        band_reach,
        long_peers,
        long_count,
        send_tile,
        features,
        query_weight,
        key_weight,
        value_weight,
        out_weight,
    )


def solution(mesh):
    return jax.shard_map(
        local,
        mesh=mesh,
        in_specs=(
            P(("grp", "rng"), None),
            P(),
            P(),
            P(),
            P(),
            P(("grp", "rng")),
            P(("grp", "rng"), None),
            P(("grp", "rng")),
            P(("grp", "rng"), None),
        ),
        out_specs=P(("grp", "rng"), None),
        check_vma=False,
    )
```

```python
import functools

import jax
import jax.numpy as jnp
from jax import lax
from jax.experimental import pallas as pl
from jax.experimental.pallas import tpu as pltpu
from jax.sharding import PartitionSpec as P

MESH = pl.DeviceIdType.MESH
F32 = jnp.float32
BF16 = jnp.bfloat16

EPSILON = 1e-06
D = 1024
ROWS = 256
TILE = 128
PORTAL = 64
MAXLONG = 6
LANES = 128
PAIRS = D // LANES
SCALE = 64 ** (-0.5)
FLOOR = -3.0e38

GRAY = {0: 0, 1: 1, 2: 3, 3: 2}
X_ORDER = ((1, 0), (3, 0), (1, 1), (3, 1), (2, 0), (2, 1))
NEAR_BLOCKS = 4
SLOTS = 16
HALO = NEAR_BLOCKS + SLOTS


def project(src, block, count, pairs, dst_block, scale=None):
    rows = count * PORTAL
    width = D // 2

    @pl.loop(0, 2, unroll=True)
    def _(step):
        columns = pl.ds(pl.multiple_of(step * width, width), width)
        for weight, dst in pairs:
            total = jnp.dot(
                src[pl.ds(block, count)].reshape(rows, D),
                weight[:, columns],
                preferred_element_type=F32,
            ).astype(BF16)
            if scale is not None:
                total = total * jnp.asarray(scale, BF16)
            dst[pl.ds(dst_block, count), :, columns] = total.reshape(count, PORTAL, width)


def kernel(
    reach_ref,
    peers_ref,
    count_ref,
    pick_ref,
    feat_hbm,
    wq_hbm,
    wk_hbm,
    wv_hbm,
    wo_hbm,
    out_ref,
    feat,
    wq,
    wk,
    wv,
    wo,
    normed,
    partner,
    partner_pick,
    arrived,
    stage_own,
    stage_far,
    queries,
    keys,
    values,
    attended,
    bias_near,
    bias_far,
    acc_near,
    sum_near,
    max_near,
    in_sem,
    send_own,
    recv_own,
    send_far,
    recv_far,
    send_y,
    recv_y,
    send_halo,
    recv_halo,
):
    g = lax.axis_index("grp")
    r = lax.axis_index("rng")
    x, row_bit, core = g // 4, (g // 2) % 2, g % 2

    def device(dx, dy, dc):
        return (
            lax.rem(x + dx, 4) * 4 + lax.rem(row_bit + dy, 2) * 2 + lax.rem(core + dc, 2),
            r,
        )

    above = (g, lax.rem(r + 1, 16))
    below = (g, lax.rem(r + 15, 16))
    row_flows = X_ORDER + ((0, 1),)

    loads = [
        pltpu.make_async_copy(src, dst, in_sem.at[i])
        for i, (src, dst) in enumerate(
            ((feat_hbm, feat), (wq_hbm, wq), (wk_hbm, wk), (wv_hbm, wv), (wo_hbm, wo))
        )
    ]
    for load in loads:
        load.start()

    barrier = pltpu.get_barrier_semaphore()
    friends = [device(dx, 0, dc) for dx, dc in row_flows] + [device(0, 1, 0), above, below]
    for friend in friends:
        pl.semaphore_signal(barrier, inc=1, device_id=friend, device_id_type=MESH)

    loads[0].wait()

    @pl.loop(0, ROWS // PORTAL)
    def _(block):
        rows = pl.ds(pl.multiple_of(block * PORTAL, PORTAL), PORTAL)
        widened = feat[rows, :].astype(F32)
        factor = lax.rsqrt(jnp.mean(widened * widened, axis=1, keepdims=True) + EPSILON)
        normed[block] = (widened * factor).astype(BF16)

    def pick_own(flow):
        dx, dc = row_flows[flow]
        target, _ = device(dx, 0, dc)
        stage_own[flow] = normed[pick_ref[0, target]]

    def slot_of_flow(dx, dc, far):
        return 8 * far + 2 * GRAY[dx] + dc

    for flow in range(len(row_flows)):
        pick_own(flow)

    pl.semaphore_wait(barrier, len(friends))

    cross = [
        pltpu.make_async_remote_copy(
            src_ref=normed, dst_ref=partner, send_sem=send_y.at[0], recv_sem=recv_y.at[0],
            device_id=device(0, 1, 0), device_id_type=MESH,
        ),
        pltpu.make_async_remote_copy(
            src_ref=pick_ref, dst_ref=partner_pick, send_sem=send_y.at[1], recv_sem=recv_y.at[1],
            device_id=device(0, 1, 0), device_id_type=MESH,
        ),
    ]
    for copy in cross:
        copy.start()
    own = []
    for flow, (dx, dc) in enumerate(row_flows):
        copy = pltpu.make_async_remote_copy(
            src_ref=stage_own.at[flow],
            dst_ref=arrived.at[slot_of_flow(dx, dc, 0)],
            send_sem=send_own.at[flow],
            recv_sem=recv_own.at[flow],
            device_id=device(dx, 0, dc),
            device_id_type=MESH,
        )
        copy.start()
        own.append(copy)

    reach = reach_ref[0]
    place_q = lax.broadcasted_iota(jnp.int32, (ROWS, ROWS), 0)
    place_k = lax.broadcasted_iota(jnp.int32, (ROWS, ROWS), 1)
    bias_near[...] = jnp.where(jnp.abs(place_q - place_k) <= reach, 0.0, -jnp.inf)
    tile_q = lax.broadcasted_iota(jnp.int32, (TILE, TILE), 0)
    tile_k = lax.broadcasted_iota(jnp.int32, (TILE, TILE), 1)
    slot_of = lax.broadcasted_iota(jnp.int32, (TILE, MAXLONG * PORTAL), 1) // PORTAL
    for tile in range(2):
        gap = (tile_q - tile_k if tile == 0 else tile_k - tile_q) + TILE
        bias_far[tile, :, :TILE] = jnp.where(gap <= reach, 0.0, -jnp.inf)
        bias_far[tile, :, TILE:] = jnp.where(slot_of < count_ref[tile], 0.0, -jnp.inf)

    loads[1].wait()
    project(normed, 0, 4, ((wq, queries),), 0, SCALE)
    loads[2].wait()
    loads[3].wait()
    project(normed, 0, 4, ((wk, keys), (wv, values)), 0)

    even = lax.broadcasted_iota(jnp.int32, (TILE, LANES), 1) < LANES // 2

    def attend(tile, lanes, key_rows, value_rows, bias):
        query = queries[pl.ds(tile * 2, 2), :, lanes].reshape(TILE, LANES)
        none = jnp.zeros_like(query)
        wide = jnp.concatenate([value_rows, jnp.ones_like(value_rows)], axis=1)
        parts = []
        for head in (jnp.where(even, query, none), jnp.where(even, none, query)):
            scores = lax.dot_general(
                head, key_rows, (((1,), (1,)), ((), ())), preferred_element_type=F32
            )
            scores = scores + bias
            highest = jnp.maximum(jnp.max(scores, axis=1, keepdims=True), FLOOR)
            weights = jnp.exp(scores - highest).astype(BF16)
            mixed = jnp.dot(weights, wide, preferred_element_type=F32)
            parts.append(
                (mixed[:, :LANES], mixed[:, LANES:], jnp.broadcast_to(highest, (TILE, LANES)))
            )
        return [jnp.where(even, first, second) for first, second in zip(*parts)]

    @pl.loop(0, PAIRS, unroll=2)
    def _(pair):
        lanes = pl.ds(pl.multiple_of(pair * LANES, LANES), LANES)
        near = pl.ds(0, NEAR_BLOCKS)
        key_rows = keys[near, :, lanes].reshape(ROWS, LANES)
        value_rows = values[near, :, lanes].reshape(ROWS, LANES)
        for tile in range(2):
            rows = pl.ds(tile * TILE, TILE)
            mixed, total, top = attend(tile, lanes, key_rows, value_rows, bias_near[rows, :])
            acc_near[rows, lanes] = mixed
            sum_near[rows, lanes] = total
            max_near[rows, lanes] = top

    for copy in cross:
        copy.wait()

    def far_rows(target):
        return partner[partner_pick[0, target]]

    far = []
    for flow, (dx, dc) in enumerate(row_flows):
        target, _ = device(dx, 0, dc)
        stage_far[flow] = far_rows(target)
    for flow, (dx, dc) in enumerate(row_flows):
        copy = pltpu.make_async_remote_copy(
            src_ref=stage_far.at[flow],
            dst_ref=arrived.at[slot_of_flow(dx, dc, 1)],
            send_sem=send_far.at[flow],
            recv_sem=recv_far.at[flow],
            device_id=device(dx, 0, dc),
            device_id_type=MESH,
        )
        copy.start()
        far.append(copy)
    edges = [
        pltpu.make_async_remote_copy(
            src_ref=normed.at[pl.ds(2, 2)], dst_ref=arrived.at[pl.ds(SLOTS, 2)],
            send_sem=send_halo.at[0], recv_sem=recv_halo.at[0],
            device_id=above, device_id_type=MESH,
        ),
        pltpu.make_async_remote_copy(
            src_ref=normed.at[pl.ds(0, 2)], dst_ref=arrived.at[pl.ds(SLOTS + 2, 2)],
            send_sem=send_halo.at[1], recv_sem=recv_halo.at[1],
            device_id=below, device_id_type=MESH,
        ),
    ]
    for copy in edges:
        copy.start()
    arrived[8] = far_rows(g)

    def project_slots(first, count):
        project(arrived, first, count, ((wk, keys), (wv, values)), NEAR_BLOCKS + first)

    for copy in own:
        copy.wait_recv()
    project_slots(1, 7)
    for flow in (6, 0, 1, 2, 3):
        far[flow].wait_recv()
    project_slots(8, 6)
    for copy in (far[4], far[5], *edges):
        copy.wait_recv()
    project_slots(14, 6)

    def slot_start(tile, entry):
        peer = peers_ref[tile, entry]
        dx = lax.rem(x + 4 - lax.div(peer, 4), 4)
        place = dx + lax.div(dx, 2) * (1 - 2 * lax.rem(dx, 2))
        other = lax.rem(lax.div(peer, 2) + row_bit, 2)
        turn = lax.rem(peer + core, 2)
        return NEAR_BLOCKS + 8 * other + 2 * place + turn

    starts = [[slot_start(tile, entry) for entry in range(MAXLONG)] for tile in range(2)]

    @pl.loop(0, PAIRS, unroll=2)
    def _(pair):
        lanes = pl.ds(pl.multiple_of(pair * LANES, LANES), LANES)
        for tile in range(2):
            rows = pl.ds(tile * TILE, TILE)
            edge = pl.ds(HALO + 2 * tile, 2)

            def gathered(ref):
                return jnp.concatenate(
                    [ref[edge, :, lanes].reshape(TILE, LANES)]
                    + [ref[start, :, lanes] for start in starts[tile]],
                    axis=0,
                )

            mixed, total, top = attend(
                tile, lanes, gathered(keys), gathered(values), bias_far[tile]
            )
            near_top = max_near[rows, lanes]
            highest = jnp.maximum(near_top, top)
            near_part = jnp.exp(near_top - highest)
            far_part = jnp.exp(top - highest)
            mixed = acc_near[rows, lanes] * near_part + mixed * far_part
            total = sum_near[rows, lanes] * near_part + total * far_part
            attended[rows, lanes] = (mixed / total).astype(BF16)

    loads[4].wait()

    @pl.loop(0, 2, unroll=True)
    def _(step):
        columns = pl.ds(pl.multiple_of(step * (D // 2), D // 2), D // 2)
        total = jnp.dot(attended[...], wo[:, columns], preferred_element_type=F32)
        out_ref[:, columns] = (feat[:, columns].astype(F32) + total).astype(BF16)

    for copy in own + far + edges:
        copy.wait_send()


def local(
    features,
    query_weight,
    key_weight,
    value_weight,
    out_weight,
    band_reach,
    long_peers,
    long_count,
    send_tile,
):
    smem = pl.BlockSpec(memory_space=pltpu.SMEM)
    hbm = pl.BlockSpec(memory_space=pl.ANY)
    flows = len(X_ORDER) + 1
    dma = pltpu.SemaphoreType.DMA
    return pl.pallas_call(
        kernel,
        name="layer",
        out_shape=jax.ShapeDtypeStruct((ROWS, D), BF16),
        in_specs=[smem] * 4 + [hbm] * 5,
        out_specs=pl.BlockSpec(memory_space=pltpu.VMEM),
        scratch_shapes=[
            pltpu.VMEM((ROWS, D), BF16),
            pltpu.VMEM((D, D), BF16),
            pltpu.VMEM((D, D), BF16),
            pltpu.VMEM((D, D), BF16),
            pltpu.VMEM((D, D), BF16),
            pltpu.VMEM((4, PORTAL, D), BF16),
            pltpu.VMEM((4, PORTAL, D), BF16),
            pltpu.SMEM((1, 16), jnp.int32),
            pltpu.VMEM((SLOTS + 4, PORTAL, D), BF16),
            pltpu.VMEM((flows, PORTAL, D), BF16),
            pltpu.VMEM((flows, PORTAL, D), BF16),
            pltpu.VMEM((4, PORTAL, D), BF16),
            pltpu.VMEM((HALO + 4, PORTAL, D), BF16),
            pltpu.VMEM((HALO + 4, PORTAL, D), BF16),
            pltpu.VMEM((ROWS, D), BF16),
            pltpu.VMEM((ROWS, ROWS), F32),
            pltpu.VMEM((2, TILE, TILE + MAXLONG * PORTAL), F32),
            pltpu.VMEM((ROWS, D), F32),
            pltpu.VMEM((ROWS, D), F32),
            pltpu.VMEM((ROWS, D), F32),
            dma((5,)),
            dma((flows,)),
            dma((flows,)),
            dma((flows,)),
            dma((flows,)),
            dma((2,)),
            dma((2,)),
            dma((2,)),
            dma((2,)),
        ],
        compiler_params=pltpu.CompilerParams(
            collective_id=0, has_side_effects=True, vmem_limit_bytes=60 * 1024 * 1024
        ),
    )(
        band_reach,
        long_peers,
        long_count,
        send_tile,
        features,
        query_weight,
        key_weight,
        value_weight,
        out_weight,
    )


def solution(mesh):
    return jax.shard_map(
        local,
        mesh=mesh,
        in_specs=(
            P(("grp", "rng"), None),
            P(),
            P(),
            P(),
            P(),
            P(("grp", "rng")),
            P(("grp", "rng"), None),
            P(("grp", "rng")),
            P(("grp", "rng"), None),
        ),
        out_specs=P(("grp", "rng"), None),
        check_vma=False,
    )
```

```python
import functools

import jax
import jax.numpy as jnp
from jax import lax
from jax.experimental import pallas as pl
from jax.experimental.pallas import tpu as pltpu
from jax.sharding import PartitionSpec as P

MESH = pl.DeviceIdType.MESH
F32 = jnp.float32
BF16 = jnp.bfloat16

EPSILON = 1e-06
D = 1024
ROWS = 256
TILE = 128
PORTAL = 64
MAXLONG = 6
LANES = 128
PAIRS = D // LANES
SCALE = 64 ** (-0.5)
FLOOR = -3.0e38

GRAY = {0: 0, 1: 1, 2: 3, 3: 2}
X_ORDER = ((1, 0), (3, 0), (1, 1), (3, 1), (2, 0), (2, 1))
NEAR_BLOCKS = 4
SLOTS = 16
HALO = NEAR_BLOCKS + SLOTS


def project(src, block, count, pairs, dst_block, scale=None):
    rows = count * PORTAL
    width = D // 2

    @pl.loop(0, 2, unroll=True)
    def _(step):
        columns = pl.ds(pl.multiple_of(step * width, width), width)
        for weight, dst in pairs:
            total = jnp.dot(
                src[pl.ds(block, count)].reshape(rows, D),
                weight[:, columns],
                preferred_element_type=F32,
            ).astype(BF16)
            if scale is not None:
                total = total * jnp.asarray(scale, BF16)
            dst[pl.ds(dst_block, count), :, columns] = total.reshape(count, PORTAL, width)


def kernel(
    reach_ref,
    peers_ref,
    count_ref,
    pick_ref,
    feat_hbm,
    wq_hbm,
    wk_hbm,
    wv_hbm,
    wo_hbm,
    out_ref,
    feat,
    wq,
    wk,
    wv,
    wo,
    normed,
    partner,
    partner_pick,
    arrived,
    stage_own,
    stage_far,
    queries,
    keys,
    values,
    attended,
    bias_near,
    bias_far,
    acc_near,
    sum_near,
    max_near,
    in_sem,
    send_own,
    recv_own,
    send_far,
    recv_far,
    send_y,
    recv_y,
    send_halo,
    recv_halo,
    ready,
):
    g = lax.axis_index("grp")
    r = lax.axis_index("rng")
    x, row_bit, core = g // 4, (g // 2) % 2, g % 2

    def device(dx, dy, dc):
        return (
            lax.rem(x + dx, 4) * 4 + lax.rem(row_bit + dy, 2) * 2 + lax.rem(core + dc, 2),
            r,
        )

    above = (g, lax.rem(r + 1, 16))
    below = (g, lax.rem(r + 15, 16))
    row_flows = X_ORDER + ((0, 1),)

    loads = [
        pltpu.make_async_copy(src, dst, in_sem.at[i])
        for i, (src, dst) in enumerate(
            ((feat_hbm, feat), (wq_hbm, wq), (wk_hbm, wk), (wv_hbm, wv), (wo_hbm, wo))
        )
    ]
    for load in loads:
        load.start()

    odd = lax.rem(r, 2)
    barrier = pltpu.get_barrier_semaphore()
    friends = [device(dx, 0, dc) for dx, dc in row_flows] + [device(0, 1, 0)]
    for friend in friends:
        pl.semaphore_signal(barrier, inc=1, device_id=friend, device_id_type=MESH)

    @pl.when(odd == 0)
    def _():
        for neighbour in (above, below):
            pl.semaphore_signal(barrier, inc=1, device_id=neighbour, device_id_type=MESH)

    loads[0].wait()

    @pl.loop(0, ROWS // PORTAL)
    def _(block):
        rows = pl.ds(pl.multiple_of(block * PORTAL, PORTAL), PORTAL)
        widened = feat[rows, :].astype(F32)
        factor = lax.rsqrt(jnp.mean(widened * widened, axis=1, keepdims=True) + EPSILON)
        normed[block] = (widened * factor).astype(BF16)

    def pick_own(flow):
        dx, dc = row_flows[flow]
        target, _ = device(dx, 0, dc)
        stage_own[flow] = normed[pick_ref[0, target]]

    def slot_of_flow(dx, dc, far):
        return 8 * far + 2 * GRAY[dx] + dc

    for flow in range(len(row_flows)):
        pick_own(flow)

    pl.semaphore_wait(barrier, len(friends) + 2 * odd)

    @pl.when(odd == 1)
    def _():
        for side, neighbour in enumerate((above, below)):
            pl.semaphore_signal(
                ready.at[side], inc=1, device_id=neighbour, device_id_type=MESH
            )

    cross = [
        pltpu.make_async_remote_copy(
            src_ref=normed, dst_ref=partner, send_sem=send_y.at[0], recv_sem=recv_y.at[0],
            device_id=device(0, 1, 0), device_id_type=MESH,
        ),
        pltpu.make_async_remote_copy(
            src_ref=pick_ref, dst_ref=partner_pick, send_sem=send_y.at[1], recv_sem=recv_y.at[1],
            device_id=device(0, 1, 0), device_id_type=MESH,
        ),
    ]
    for copy in cross:
        copy.start()
    own = []
    for flow, (dx, dc) in enumerate(row_flows):
        copy = pltpu.make_async_remote_copy(
            src_ref=stage_own.at[flow],
            dst_ref=arrived.at[slot_of_flow(dx, dc, 0)],
            send_sem=send_own.at[flow],
            recv_sem=recv_own.at[flow],
            device_id=device(dx, 0, dc),
            device_id_type=MESH,
        )
        copy.start()
        own.append(copy)

    reach = reach_ref[0]
    place_q = lax.broadcasted_iota(jnp.int32, (ROWS, ROWS), 0)
    place_k = lax.broadcasted_iota(jnp.int32, (ROWS, ROWS), 1)
    bias_near[...] = jnp.where(jnp.abs(place_q - place_k) <= reach, 0.0, -jnp.inf)
    tile_q = lax.broadcasted_iota(jnp.int32, (TILE, TILE), 0)
    tile_k = lax.broadcasted_iota(jnp.int32, (TILE, TILE), 1)
    slot_of = lax.broadcasted_iota(jnp.int32, (TILE, MAXLONG * PORTAL), 1) // PORTAL
    for tile in range(2):
        gap = (tile_q - tile_k if tile == 0 else tile_k - tile_q) + TILE
        bias_far[tile, :, :TILE] = jnp.where(gap <= reach, 0.0, -jnp.inf)
        bias_far[tile, :, TILE:] = jnp.where(slot_of < count_ref[tile], 0.0, -jnp.inf)

    loads[1].wait()
    project(normed, 0, 4, ((wq, queries),), 0, SCALE)
    loads[2].wait()
    loads[3].wait()
    project(normed, 0, 4, ((wk, keys), (wv, values)), 0)

    even = lax.broadcasted_iota(jnp.int32, (TILE, LANES), 1) < LANES // 2

    def attend(tile, lanes, key_rows, value_rows, bias):
        query = queries[pl.ds(tile * 2, 2), :, lanes].reshape(TILE, LANES)
        none = jnp.zeros_like(query)
        wide = jnp.concatenate([value_rows, jnp.ones_like(value_rows)], axis=1)
        parts = []
        for head in (jnp.where(even, query, none), jnp.where(even, none, query)):
            scores = lax.dot_general(
                head, key_rows, (((1,), (1,)), ((), ())), preferred_element_type=F32
            )
            scores = scores + bias
            highest = jnp.maximum(jnp.max(scores, axis=1, keepdims=True), FLOOR)
            weights = jnp.exp(scores - highest).astype(BF16)
            mixed = jnp.dot(weights, wide, preferred_element_type=F32)
            parts.append(
                (mixed[:, :LANES], mixed[:, LANES:], jnp.broadcast_to(highest, (TILE, LANES)))
            )
        return [jnp.where(even, first, second) for first, second in zip(*parts)]

    @pl.loop(0, PAIRS, unroll=2)
    def _(pair):
        lanes = pl.ds(pl.multiple_of(pair * LANES, LANES), LANES)
        near = pl.ds(0, NEAR_BLOCKS)
        key_rows = keys[near, :, lanes].reshape(ROWS, LANES)
        value_rows = values[near, :, lanes].reshape(ROWS, LANES)
        for tile in range(2):
            rows = pl.ds(tile * TILE, TILE)
            mixed, total, top = attend(tile, lanes, key_rows, value_rows, bias_near[rows, :])
            acc_near[rows, lanes] = mixed
            sum_near[rows, lanes] = total
            max_near[rows, lanes] = top

    for copy in cross:
        copy.wait()

    def far_rows(target):
        return partner[partner_pick[0, target]]

    far = []
    for flow, (dx, dc) in enumerate(row_flows):
        target, _ = device(dx, 0, dc)
        stage_far[flow] = far_rows(target)
    for flow, (dx, dc) in enumerate(row_flows):
        copy = pltpu.make_async_remote_copy(
            src_ref=stage_far.at[flow],
            dst_ref=arrived.at[slot_of_flow(dx, dc, 1)],
            send_sem=send_far.at[flow],
            recv_sem=recv_far.at[flow],
            device_id=device(dx, 0, dc),
            device_id_type=MESH,
        )
        copy.start()
        far.append(copy)
    edges = [
        pltpu.make_async_remote_copy(
            src_ref=normed.at[pl.ds(2, 2)], dst_ref=arrived.at[pl.ds(SLOTS, 2)],
            send_sem=send_halo.at[0], recv_sem=recv_halo.at[0],
            device_id=above, device_id_type=MESH,
        ),
        pltpu.make_async_remote_copy(
            src_ref=normed.at[pl.ds(0, 2)], dst_ref=arrived.at[pl.ds(SLOTS + 2, 2)],
            send_sem=send_halo.at[1], recv_sem=recv_halo.at[1],
            device_id=below, device_id_type=MESH,
        ),
    ]
    @pl.when(odd == 0)
    def _():
        for side in range(2):
            pl.semaphore_wait(ready.at[side], 1)

    @pl.when(r != 0)
    def _():
        for copy in edges:
            copy.start()

    arrived[8] = far_rows(g)

    def project_slots(first, count):
        project(arrived, first, count, ((wk, keys), (wv, values)), NEAR_BLOCKS + first)

    for copy in own:
        copy.wait_recv()
    project_slots(1, 7)
    @pl.when(r == 0)
    def _():
        for copy in edges:
            copy.start()

    for flow in (6, 0, 1, 2, 3):
        far[flow].wait_recv()
    project_slots(8, 6)
    for copy in (far[4], far[5], *edges):
        copy.wait_recv()
    project_slots(14, 6)

    def slot_start(tile, entry):
        peer = peers_ref[tile, entry]
        dx = lax.rem(x + 4 - lax.div(peer, 4), 4)
        place = dx + lax.div(dx, 2) * (1 - 2 * lax.rem(dx, 2))
        other = lax.rem(lax.div(peer, 2) + row_bit, 2)
        turn = lax.rem(peer + core, 2)
        return NEAR_BLOCKS + 8 * other + 2 * place + turn

    starts = [[slot_start(tile, entry) for entry in range(MAXLONG)] for tile in range(2)]

    @pl.loop(0, PAIRS, unroll=2)
    def _(pair):
        lanes = pl.ds(pl.multiple_of(pair * LANES, LANES), LANES)
        for tile in range(2):
            rows = pl.ds(tile * TILE, TILE)
            edge = pl.ds(HALO + 2 * tile, 2)

            def gathered(ref):
                return jnp.concatenate(
                    [ref[edge, :, lanes].reshape(TILE, LANES)]
                    + [ref[start, :, lanes] for start in starts[tile]],
                    axis=0,
                )

            mixed, total, top = attend(
                tile, lanes, gathered(keys), gathered(values), bias_far[tile]
            )
            near_top = max_near[rows, lanes]
            highest = jnp.maximum(near_top, top)
            near_part = jnp.exp(near_top - highest)
            far_part = jnp.exp(top - highest)
            mixed = acc_near[rows, lanes] * near_part + mixed * far_part
            total = sum_near[rows, lanes] * near_part + total * far_part
            attended[rows, lanes] = (mixed / total).astype(BF16)

    loads[4].wait()

    @pl.loop(0, 2, unroll=True)
    def _(step):
        columns = pl.ds(pl.multiple_of(step * (D // 2), D // 2), D // 2)
        total = jnp.dot(attended[...], wo[:, columns], preferred_element_type=F32)
        out_ref[:, columns] = (feat[:, columns].astype(F32) + total).astype(BF16)

    for copy in own + far + edges:
        copy.wait_send()


def local(
    features,
    query_weight,
    key_weight,
    value_weight,
    out_weight,
    band_reach,
    long_peers,
    long_count,
    send_tile,
):
    smem = pl.BlockSpec(memory_space=pltpu.SMEM)
    hbm = pl.BlockSpec(memory_space=pl.ANY)
    flows = len(X_ORDER) + 1
    dma = pltpu.SemaphoreType.DMA
    return pl.pallas_call(
        kernel,
        name="layer",
        out_shape=jax.ShapeDtypeStruct((ROWS, D), BF16),
        in_specs=[smem] * 4 + [hbm] * 5,
        out_specs=pl.BlockSpec(memory_space=pltpu.VMEM),
        scratch_shapes=[
            pltpu.VMEM((ROWS, D), BF16),
            pltpu.VMEM((D, D), BF16),
            pltpu.VMEM((D, D), BF16),
            pltpu.VMEM((D, D), BF16),
            pltpu.VMEM((D, D), BF16),
            pltpu.VMEM((4, PORTAL, D), BF16),
            pltpu.VMEM((4, PORTAL, D), BF16),
            pltpu.SMEM((1, 16), jnp.int32),
            pltpu.VMEM((SLOTS + 4, PORTAL, D), BF16),
            pltpu.VMEM((flows, PORTAL, D), BF16),
            pltpu.VMEM((flows, PORTAL, D), BF16),
            pltpu.VMEM((4, PORTAL, D), BF16),
            pltpu.VMEM((HALO + 4, PORTAL, D), BF16),
            pltpu.VMEM((HALO + 4, PORTAL, D), BF16),
            pltpu.VMEM((ROWS, D), BF16),
            pltpu.VMEM((ROWS, ROWS), F32),
            pltpu.VMEM((2, TILE, TILE + MAXLONG * PORTAL), F32),
            pltpu.VMEM((ROWS, D), F32),
            pltpu.VMEM((ROWS, D), F32),
            pltpu.VMEM((ROWS, D), F32),
            dma((5,)),
            dma((flows,)),
            dma((flows,)),
            dma((flows,)),
            dma((flows,)),
            dma((2,)),
            dma((2,)),
            dma((2,)),
            dma((2,)),
            pltpu.SemaphoreType.REGULAR((2,)),
        ],
        compiler_params=pltpu.CompilerParams(
            collective_id=0, has_side_effects=True, vmem_limit_bytes=60 * 1024 * 1024
        ),
    )(
        band_reach,
        long_peers,
        long_count,
        send_tile,
        features,
        query_weight,
        key_weight,
        value_weight,
        out_weight,
    )


def solution(mesh):
    return jax.shard_map(
        local,
        mesh=mesh,
        in_specs=(
            P(("grp", "rng"), None),
            P(),
            P(),
            P(),
            P(),
            P(("grp", "rng")),
            P(("grp", "rng"), None),
            P(("grp", "rng")),
            P(("grp", "rng"), None),
        ),
        out_specs=P(("grp", "rng"), None),
        check_vma=False,
    )
```

```python
import functools

import jax
import jax.numpy as jnp
from jax import lax
from jax.experimental import pallas as pl
from jax.experimental.pallas import tpu as pltpu
from jax.sharding import PartitionSpec as P

MESH = pl.DeviceIdType.MESH
F32 = jnp.float32
BF16 = jnp.bfloat16

EPSILON = 1e-06
D = 1024
ROWS = 256
TILE = 128
PORTAL = 64
MAXLONG = 6
LANES = 128
PAIRS = D // LANES
SCALE = 64 ** (-0.5)
FLOOR = -3.0e38

GRAY = {0: 0, 1: 1, 2: 3, 3: 2}
X_ORDER = ((1, 0), (3, 0), (1, 1), (3, 1), (2, 0), (2, 1))
NEAR_BLOCKS = 4
SLOTS = 16
HALO = NEAR_BLOCKS + SLOTS


def project(src, block, count, pairs, dst_block, scale=None):
    rows = count * PORTAL
    width = D // 2

    @pl.loop(0, 2, unroll=True)
    def _(step):
        columns = pl.ds(pl.multiple_of(step * width, width), width)
        for weight, dst in pairs:
            total = jnp.dot(
                src[pl.ds(block, count)].reshape(rows, D),
                weight[:, columns],
                preferred_element_type=F32,
            ).astype(BF16)
            if scale is not None:
                total = total * jnp.asarray(scale, BF16)
            dst[pl.ds(dst_block, count), :, columns] = total.reshape(count, PORTAL, width)


def kernel(
    reach_hbm,
    peers_hbm,
    count_hbm,
    pick_hbm,
    feat_hbm,
    wq_hbm,
    wk_hbm,
    wv_hbm,
    out_ref,
    reach_ref,
    peers_ref,
    count_ref,
    pick_ref,
    feat,
    wq,
    wk,
    wv,
    normed,
    partner,
    partner_pick,
    arrived,
    stage_own,
    stage_far,
    queries,
    keys,
    values,
    bias_near,
    bias_far,
    acc_near,
    sum_near,
    max_near,
    in_sem,
    send_own,
    recv_own,
    send_far,
    recv_far,
    send_y,
    recv_y,
    send_halo,
    recv_halo,
    ready,
):
    g = lax.axis_index("grp")
    r = lax.axis_index("rng")
    x, row_bit, core = g // 4, (g // 2) % 2, g % 2

    def device(dx, dy, dc):
        return (
            lax.rem(x + dx, 4) * 4 + lax.rem(row_bit + dy, 2) * 2 + lax.rem(core + dc, 2),
            r,
        )

    above = (g, lax.rem(r + 1, 16))
    below = (g, lax.rem(r + 15, 16))
    row_flows = X_ORDER + ((0, 1),)

    def loads_of(first, *pairs):
        return [
            pltpu.make_async_copy(src, dst, in_sem.at[first + i])
            for i, (src, dst) in enumerate(pairs)
        ]

    feat_load, pick_load, *small_loads = loads_of(
        0,
        (feat_hbm, feat),
        (pick_hbm, pick_ref),
        (reach_hbm, reach_ref),
        (peers_hbm, peers_ref),
        (count_hbm, count_ref),
    )
    loads = loads_of(5, (wq_hbm, wq), (wk_hbm, wk), (wv_hbm, wv))
    for load in (feat_load, pick_load, *small_loads):
        load.start()

    odd = lax.rem(r, 2)
    barrier = pltpu.get_barrier_semaphore()
    friends = [device(dx, 0, dc) for dx, dc in row_flows] + [device(0, 1, 0)]
    for friend in friends:
        pl.semaphore_signal(barrier, inc=1, device_id=friend, device_id_type=MESH)

    @pl.when(odd == 0)
    def _():
        for neighbour in (above, below):
            pl.semaphore_signal(barrier, inc=1, device_id=neighbour, device_id_type=MESH)

    feat_load.wait()
    for load in loads:
        load.start()

    @pl.loop(0, ROWS // PORTAL)
    def _(block):
        rows = pl.ds(pl.multiple_of(block * PORTAL, PORTAL), PORTAL)
        widened = feat[rows, :].astype(F32)
        factor = lax.rsqrt(jnp.mean(widened * widened, axis=1, keepdims=True) + EPSILON)
        normed[block] = (widened * factor).astype(BF16)

    def slot_of_flow(dx, dc, far):
        return 8 * far + 2 * GRAY[dx] + dc

    pick_load.wait()
    pl.semaphore_wait(barrier, len(friends) + 2 * odd)

    @pl.when(odd == 1)
    def _():
        for side, neighbour in enumerate((above, below)):
            pl.semaphore_signal(
                ready.at[side], inc=1, device_id=neighbour, device_id_type=MESH
            )

    cross = [
        pltpu.make_async_remote_copy(
            src_ref=normed, dst_ref=partner, send_sem=send_y.at[0], recv_sem=recv_y.at[0],
            device_id=device(0, 1, 0), device_id_type=MESH,
        ),
        pltpu.make_async_remote_copy(
            src_ref=pick_ref, dst_ref=partner_pick, send_sem=send_y.at[1], recv_sem=recv_y.at[1],
            device_id=device(0, 1, 0), device_id_type=MESH,
        ),
    ]
    for copy in cross:
        copy.start()
    own = []
    for flow, (dx, dc) in enumerate(row_flows):
        target, _ = device(dx, 0, dc)
        stage_own[flow] = normed[pick_ref[0, target]]
        copy = pltpu.make_async_remote_copy(
            src_ref=stage_own.at[flow],
            dst_ref=arrived.at[slot_of_flow(dx, dc, 0)],
            send_sem=send_own.at[flow],
            recv_sem=recv_own.at[flow],
            device_id=device(dx, 0, dc),
            device_id_type=MESH,
        )
        copy.start()
        own.append(copy)

    for load in small_loads:
        load.wait()
    reach = reach_ref[0]
    place_q = lax.broadcasted_iota(jnp.int32, (ROWS, ROWS), 0)
    place_k = lax.broadcasted_iota(jnp.int32, (ROWS, ROWS), 1)
    bias_near[...] = jnp.where(jnp.abs(place_q - place_k) <= reach, 0.0, -jnp.inf)
    tile_q = lax.broadcasted_iota(jnp.int32, (TILE, TILE), 0)
    tile_k = lax.broadcasted_iota(jnp.int32, (TILE, TILE), 1)
    slot_of = lax.broadcasted_iota(jnp.int32, (TILE, MAXLONG * PORTAL), 1) // PORTAL
    for tile in range(2):
        gap = (tile_q - tile_k if tile == 0 else tile_k - tile_q) + TILE
        bias_far[tile, :, :TILE] = jnp.where(gap <= reach, 0.0, -jnp.inf)
        bias_far[tile, :, TILE:] = jnp.where(slot_of < count_ref[tile], 0.0, -jnp.inf)

    loads[0].wait()
    project(normed, 0, 4, ((wq, queries),), 0, SCALE)
    loads[1].wait()
    loads[2].wait()
    project(normed, 0, 4, ((wk, keys), (wv, values)), 0)

    even = lax.broadcasted_iota(jnp.int32, (TILE, LANES), 1) < LANES // 2

    def attend(tile, lanes, key_rows, value_rows, bias):
        query = queries[pl.ds(tile * 2, 2), :, lanes].reshape(TILE, LANES)
        none = jnp.zeros_like(query)
        wide = jnp.concatenate([value_rows, jnp.ones_like(value_rows)], axis=1)
        parts = []
        for head in (jnp.where(even, query, none), jnp.where(even, none, query)):
            scores = lax.dot_general(
                head, key_rows, (((1,), (1,)), ((), ())), preferred_element_type=F32
            )
            scores = scores + bias
            highest = jnp.maximum(jnp.max(scores, axis=1, keepdims=True), FLOOR)
            weights = jnp.exp(scores - highest).astype(BF16)
            mixed = jnp.dot(weights, wide, preferred_element_type=F32)
            parts.append(
                (mixed[:, :LANES], mixed[:, LANES:], jnp.broadcast_to(highest, (TILE, LANES)))
            )
        return [jnp.where(even, first, second) for first, second in zip(*parts)]

    @pl.loop(0, PAIRS, unroll=2)
    def _(pair):
        lanes = pl.ds(pl.multiple_of(pair * LANES, LANES), LANES)
        near = pl.ds(0, NEAR_BLOCKS)
        key_rows = keys[near, :, lanes].reshape(ROWS, LANES)
        value_rows = values[near, :, lanes].reshape(ROWS, LANES)
        for tile in range(2):
            rows = pl.ds(tile * TILE, TILE)
            mixed, total, top = attend(tile, lanes, key_rows, value_rows, bias_near[rows, :])
            acc_near[rows, lanes] = mixed
            sum_near[rows, lanes] = total
            max_near[rows, lanes] = top

    for copy in cross:
        copy.wait()

    def far_rows(target):
        return partner[partner_pick[0, target]]

    far = []
    for flow, (dx, dc) in enumerate(row_flows):
        target, _ = device(dx, 0, dc)
        stage_far[flow] = far_rows(target)
        copy = pltpu.make_async_remote_copy(
            src_ref=stage_far.at[flow],
            dst_ref=arrived.at[slot_of_flow(dx, dc, 1)],
            send_sem=send_far.at[flow],
            recv_sem=recv_far.at[flow],
            device_id=device(dx, 0, dc),
            device_id_type=MESH,
        )
        copy.start()
        far.append(copy)
    edges = [
        pltpu.make_async_remote_copy(
            src_ref=normed.at[pl.ds(2, 2)], dst_ref=arrived.at[pl.ds(SLOTS, 2)],
            send_sem=send_halo.at[0], recv_sem=recv_halo.at[0],
            device_id=above, device_id_type=MESH,
        ),
        pltpu.make_async_remote_copy(
            src_ref=normed.at[pl.ds(0, 2)], dst_ref=arrived.at[pl.ds(SLOTS + 2, 2)],
            send_sem=send_halo.at[1], recv_sem=recv_halo.at[1],
            device_id=below, device_id_type=MESH,
        ),
    ]
    @pl.when(odd == 0)
    def _():
        for side in range(2):
            pl.semaphore_wait(ready.at[side], 1)

    @pl.when(r != 0)
    def _():
        for copy in edges:
            copy.start()

    arrived[8] = far_rows(g)

    def project_slots(first, count):
        project(arrived, first, count, ((wk, keys), (wv, values)), NEAR_BLOCKS + first)

    for copy in own:
        copy.wait_recv()
    project_slots(1, 7)
    @pl.when(r == 0)
    def _():
        for copy in edges:
            copy.start()

    for flow in (6, 0, 1, 2, 3):
        far[flow].wait_recv()
    project_slots(8, 6)
    for copy in (far[4], far[5], *edges):
        copy.wait_recv()
    project_slots(14, 6)

    def slot_start(tile, entry):
        peer = peers_ref[tile, entry]
        dx = lax.rem(x + 4 - lax.div(peer, 4), 4)
        place = dx + lax.div(dx, 2) * (1 - 2 * lax.rem(dx, 2))
        other = lax.rem(lax.div(peer, 2) + row_bit, 2)
        turn = lax.rem(peer + core, 2)
        return NEAR_BLOCKS + 8 * other + 2 * place + turn

    starts = [[slot_start(tile, entry) for entry in range(MAXLONG)] for tile in range(2)]

    @pl.loop(0, PAIRS, unroll=4)
    def _(pair):
        lanes = pl.ds(pl.multiple_of(pair * LANES, LANES), LANES)
        for tile in range(2):
            rows = pl.ds(tile * TILE, TILE)
            edge = pl.ds(HALO + 2 * tile, 2)

            def gathered(ref):
                return jnp.concatenate(
                    [ref[edge, :, lanes].reshape(TILE, LANES)]
                    + [ref[start, :, lanes] for start in starts[tile]],
                    axis=0,
                )

            mixed, total, top = attend(
                tile, lanes, gathered(keys), gathered(values), bias_far[tile]
            )
            near_top = max_near[rows, lanes]
            highest = jnp.maximum(near_top, top)
            near_part = jnp.exp(near_top - highest)
            far_part = jnp.exp(top - highest)
            mixed = acc_near[rows, lanes] * near_part + mixed * far_part
            total = sum_near[rows, lanes] * near_part + total * far_part
            out_ref[rows, lanes] = (mixed / total).astype(BF16)

    for copy in own + far + edges:
        copy.wait_send()


def local(
    features,
    query_weight,
    key_weight,
    value_weight,
    out_weight,
    band_reach,
    long_peers,
    long_count,
    send_tile,
):
    hbm = pl.BlockSpec(memory_space=pltpu.HBM)
    flows = len(X_ORDER) + 1
    dma = pltpu.SemaphoreType.DMA
    attended = pl.pallas_call(
        kernel,
        name="layer",
        out_shape=jax.ShapeDtypeStruct((ROWS, D), BF16),
        in_specs=[hbm] * 8,
        out_specs=pl.BlockSpec(memory_space=pltpu.VMEM),
        scratch_shapes=[
            pltpu.SMEM((1,), jnp.int32),
            pltpu.SMEM((2, MAXLONG), jnp.int32),
            pltpu.SMEM((2,), jnp.int32),
            pltpu.SMEM((1, 16), jnp.int32),
            pltpu.VMEM((ROWS, D), BF16),
            pltpu.VMEM((D, D), BF16),
            pltpu.VMEM((D, D), BF16),
            pltpu.VMEM((D, D), BF16),
            pltpu.VMEM((4, PORTAL, D), BF16),
            pltpu.VMEM((4, PORTAL, D), BF16),
            pltpu.SMEM((1, 16), jnp.int32),
            pltpu.VMEM((SLOTS + 4, PORTAL, D), BF16),
            pltpu.VMEM((flows, PORTAL, D), BF16),
            pltpu.VMEM((flows, PORTAL, D), BF16),
            pltpu.VMEM((4, PORTAL, D), BF16),
            pltpu.VMEM((HALO + 4, PORTAL, D), BF16),
            pltpu.VMEM((HALO + 4, PORTAL, D), BF16),
            pltpu.VMEM((ROWS, ROWS), F32),
            pltpu.VMEM((2, TILE, TILE + MAXLONG * PORTAL), F32),
            pltpu.VMEM((ROWS, D), F32),
            pltpu.VMEM((ROWS, D), F32),
            pltpu.VMEM((ROWS, D), F32),
            dma((8,)),
            dma((flows,)),
            dma((flows,)),
            dma((flows,)),
            dma((flows,)),
            dma((2,)),
            dma((2,)),
            dma((2,)),
            dma((2,)),
            pltpu.SemaphoreType.REGULAR((2,)),
        ],
        compiler_params=pltpu.CompilerParams(
            collective_id=0, has_side_effects=True, vmem_limit_bytes=56 * 1024 * 1024
        ),
    )(
        band_reach,
        long_peers,
        long_count,
        send_tile,
        features,
        query_weight,
        key_weight,
        value_weight,
    )
    projected = jnp.dot(attended, out_weight, preferred_element_type=F32)
    return (features.astype(F32) + projected).astype(BF16)


def solution(mesh):
    return jax.shard_map(
        local,
        mesh=mesh,
        in_specs=(
            P(("grp", "rng"), None),
            P(),
            P(),
            P(),
            P(),
            P(("grp", "rng")),
            P(("grp", "rng"), None),
            P(("grp", "rng")),
            P(("grp", "rng"), None),
        ),
        out_specs=P(("grp", "rng"), None),
        check_vma=False,
    )
```

```python
import functools

import jax
import jax.numpy as jnp
from jax import lax
from jax.experimental import pallas as pl
from jax.experimental.pallas import tpu as pltpu
from jax.sharding import PartitionSpec as P

MESH = pl.DeviceIdType.MESH
F32 = jnp.float32
BF16 = jnp.bfloat16

EPSILON = 1e-06
D = 1024
ROWS = 256
TILE = 128
PORTAL = 64
MAXLONG = 6
LANES = 128
PAIRS = D // LANES
SCALE = 64 ** (-0.5)
FLOOR = -3.0e38

GRAY = {0: 0, 1: 1, 2: 3, 3: 2}
X_ORDER = ((1, 0), (3, 0), (1, 1), (3, 1), (2, 0), (2, 1))
NEAR_BLOCKS = 4
SLOTS = 16
HALO = NEAR_BLOCKS + SLOTS


def project(src, block, count, pairs, dst_block, scale=None):
    rows = count * PORTAL
    width = D // 2

    @pl.loop(0, 2, unroll=True)
    def _(step):
        columns = pl.ds(pl.multiple_of(step * width, width), width)
        for weight, dst in pairs:
            total = jnp.dot(
                src[pl.ds(block, count)].reshape(rows, D),
                weight[:, columns],
                preferred_element_type=F32,
            ).astype(BF16)
            if scale is not None:
                total = total * jnp.asarray(scale, BF16)
            dst[pl.ds(dst_block, count), :, columns] = total.reshape(count, PORTAL, width)


def kernel(
    reach_ref,
    peers_hbm,
    count_hbm,
    pick_hbm,
    feat_hbm,
    wq_hbm,
    wk_hbm,
    wv_hbm,
    out_ref,
    peers_ref,
    count_ref,
    pick_ref,
    feat,
    wq,
    wk,
    wv,
    normed,
    partner,
    partner_pick,
    arrived,
    stage_own,
    stage_far,
    queries,
    keys,
    values,
    bias_near,
    bias_far,
    acc_near,
    sum_near,
    max_near,
    in_sem,
    send_own,
    recv_own,
    send_far,
    recv_far,
    send_y,
    recv_y,
    send_halo,
    recv_halo,
    ready,
):
    g = lax.axis_index("grp")
    r = lax.axis_index("rng")
    x, row_bit, core = g // 4, (g // 2) % 2, g % 2

    def device(dx, dy, dc):
        return (
            lax.rem(x + dx, 4) * 4 + lax.rem(row_bit + dy, 2) * 2 + lax.rem(core + dc, 2),
            r,
        )

    above = (g, lax.rem(r + 1, 16))
    below = (g, lax.rem(r + 15, 16))
    row_flows = X_ORDER + ((0, 1),)

    def loads_of(first, *pairs):
        return [
            pltpu.make_async_copy(src, dst, in_sem.at[first + i])
            for i, (src, dst) in enumerate(pairs)
        ]

    feat_load, pick_load, *small_loads = loads_of(
        0,
        (feat_hbm, feat),
        (pick_hbm, pick_ref),
        (peers_hbm, peers_ref),
        (count_hbm, count_ref),
    )
    loads = loads_of(4, (wq_hbm, wq), (wk_hbm, wk), (wv_hbm, wv))
    for load in (feat_load, pick_load, *small_loads):
        load.start()

    odd = lax.rem(r, 2)
    barrier = pltpu.get_barrier_semaphore()
    friends = [device(dx, 0, dc) for dx, dc in row_flows] + [device(0, 1, 0)]
    for friend in friends:
        pl.semaphore_signal(barrier, inc=1, device_id=friend, device_id_type=MESH)

    @pl.when(odd == 0)
    def _():
        for neighbour in (above, below):
            pl.semaphore_signal(barrier, inc=1, device_id=neighbour, device_id_type=MESH)

    feat_load.wait()
    for load in loads:
        load.start()

    @pl.loop(0, ROWS // PORTAL)
    def _(block):
        rows = pl.ds(pl.multiple_of(block * PORTAL, PORTAL), PORTAL)
        widened = feat[rows, :].astype(F32)
        factor = lax.rsqrt(jnp.mean(widened * widened, axis=1, keepdims=True) + EPSILON)
        normed[block] = (widened * factor).astype(BF16)

    def slot_of_flow(dx, dc, far):
        return 8 * far + 2 * GRAY[dx] + dc

    pick_load.wait()
    pl.semaphore_wait(barrier, len(friends) + 2 * odd)

    @pl.when(odd == 1)
    def _():
        for side, neighbour in enumerate((above, below)):
            pl.semaphore_signal(
                ready.at[side], inc=1, device_id=neighbour, device_id_type=MESH
            )

    cross = [
        pltpu.make_async_remote_copy(
            src_ref=normed, dst_ref=partner, send_sem=send_y.at[0], recv_sem=recv_y.at[0],
            device_id=device(0, 1, 0), device_id_type=MESH,
        ),
        pltpu.make_async_remote_copy(
            src_ref=pick_ref, dst_ref=partner_pick, send_sem=send_y.at[1], recv_sem=recv_y.at[1],
            device_id=device(0, 1, 0), device_id_type=MESH,
        ),
    ]
    for copy in cross:
        copy.start()
    own = []
    for flow, (dx, dc) in enumerate(row_flows):
        target, _ = device(dx, 0, dc)
        stage_own[flow] = normed[pick_ref[0, target]]
        copy = pltpu.make_async_remote_copy(
            src_ref=stage_own.at[flow],
            dst_ref=arrived.at[slot_of_flow(dx, dc, 0)],
            send_sem=send_own.at[flow],
            recv_sem=recv_own.at[flow],
            device_id=device(dx, 0, dc),
            device_id_type=MESH,
        )
        copy.start()
        own.append(copy)

    for load in small_loads:
        load.wait()
    reach = reach_ref[0]
    place_q = lax.broadcasted_iota(jnp.int32, (ROWS, ROWS), 0)
    place_k = lax.broadcasted_iota(jnp.int32, (ROWS, ROWS), 1)
    bias_near[...] = jnp.where(jnp.abs(place_q - place_k) <= reach, 0.0, -jnp.inf)
    tile_q = lax.broadcasted_iota(jnp.int32, (TILE, TILE), 0)
    tile_k = lax.broadcasted_iota(jnp.int32, (TILE, TILE), 1)
    slot_of = lax.broadcasted_iota(jnp.int32, (TILE, MAXLONG * PORTAL), 1) // PORTAL
    for tile in range(2):
        gap = (tile_q - tile_k if tile == 0 else tile_k - tile_q) + TILE
        bias_far[tile, :, :TILE] = jnp.where(gap <= reach, 0.0, -jnp.inf)
        bias_far[tile, :, TILE:] = jnp.where(slot_of < count_ref[tile], 0.0, -jnp.inf)

    loads[0].wait()
    project(normed, 0, 4, ((wq, queries),), 0, SCALE)
    loads[1].wait()
    loads[2].wait()
    project(normed, 0, 4, ((wk, keys), (wv, values)), 0)

    even = lax.broadcasted_iota(jnp.int32, (TILE, LANES), 1) < LANES // 2

    def attend(tile, lanes, key_rows, value_rows, bias):
        query = queries[pl.ds(tile * 2, 2), :, lanes].reshape(TILE, LANES)
        none = jnp.zeros_like(query)
        wide = jnp.concatenate([value_rows, jnp.ones_like(value_rows)], axis=1)
        parts = []
        for head in (jnp.where(even, query, none), jnp.where(even, none, query)):
            scores = lax.dot_general(
                head, key_rows, (((1,), (1,)), ((), ())), preferred_element_type=F32
            )
            scores = scores + bias
            highest = jnp.maximum(jnp.max(scores, axis=1, keepdims=True), FLOOR)
            weights = jnp.exp(scores - highest).astype(BF16)
            mixed = jnp.dot(weights, wide, preferred_element_type=F32)
            parts.append(
                (mixed[:, :LANES], mixed[:, LANES:], jnp.broadcast_to(highest, (TILE, LANES)))
            )
        return [jnp.where(even, first, second) for first, second in zip(*parts)]

    @pl.loop(0, PAIRS, unroll=2)
    def _(pair):
        lanes = pl.ds(pl.multiple_of(pair * LANES, LANES), LANES)
        near = pl.ds(0, NEAR_BLOCKS)
        key_rows = keys[near, :, lanes].reshape(ROWS, LANES)
        value_rows = values[near, :, lanes].reshape(ROWS, LANES)
        for tile in range(2):
            rows = pl.ds(tile * TILE, TILE)
            mixed, total, top = attend(tile, lanes, key_rows, value_rows, bias_near[rows, :])
            acc_near[rows, lanes] = mixed
            sum_near[rows, lanes] = total
            max_near[rows, lanes] = top

    for copy in cross:
        copy.wait()

    def far_rows(target):
        return partner[partner_pick[0, target]]

    far = []
    for flow, (dx, dc) in enumerate(row_flows):
        target, _ = device(dx, 0, dc)
        stage_far[flow] = far_rows(target)
        copy = pltpu.make_async_remote_copy(
            src_ref=stage_far.at[flow],
            dst_ref=arrived.at[slot_of_flow(dx, dc, 1)],
            send_sem=send_far.at[flow],
            recv_sem=recv_far.at[flow],
            device_id=device(dx, 0, dc),
            device_id_type=MESH,
        )
        copy.start()
        far.append(copy)
    edges = [
        pltpu.make_async_remote_copy(
            src_ref=normed.at[pl.ds(2, 2)], dst_ref=arrived.at[pl.ds(SLOTS, 2)],
            send_sem=send_halo.at[0], recv_sem=recv_halo.at[0],
            device_id=above, device_id_type=MESH,
        ),
        pltpu.make_async_remote_copy(
            src_ref=normed.at[pl.ds(0, 2)], dst_ref=arrived.at[pl.ds(SLOTS + 2, 2)],
            send_sem=send_halo.at[1], recv_sem=recv_halo.at[1],
            device_id=below, device_id_type=MESH,
        ),
    ]
    @pl.when(odd == 0)
    def _():
        for side in range(2):
            pl.semaphore_wait(ready.at[side], 1)

    @pl.when(r != 0)
    def _():
        for copy in edges:
            copy.start()

    arrived[8] = far_rows(g)

    def project_slots(first, count):
        project(arrived, first, count, ((wk, keys), (wv, values)), NEAR_BLOCKS + first)

    for copy in own:
        copy.wait_recv()
    project_slots(1, 7)
    @pl.when(r == 0)
    def _():
        for copy in edges:
            copy.start()

    for flow in (6, 0, 1, 2, 3):
        far[flow].wait_recv()
    project_slots(8, 6)
    for copy in (far[4], far[5], *edges):
        copy.wait_recv()
    project_slots(14, 6)

    def slot_start(tile, entry):
        peer = peers_ref[tile, entry]
        dx = lax.rem(x + 4 - lax.div(peer, 4), 4)
        place = dx + lax.div(dx, 2) * (1 - 2 * lax.rem(dx, 2))
        other = lax.rem(lax.div(peer, 2) + row_bit, 2)
        turn = lax.rem(peer + core, 2)
        return NEAR_BLOCKS + 8 * other + 2 * place + turn

    starts = [[slot_start(tile, entry) for entry in range(MAXLONG)] for tile in range(2)]

    @pl.loop(0, PAIRS, unroll=4)
    def _(pair):
        lanes = pl.ds(pl.multiple_of(pair * LANES, LANES), LANES)
        for tile in range(2):
            rows = pl.ds(tile * TILE, TILE)
            edge = pl.ds(HALO + 2 * tile, 2)

            def gathered(ref):
                return jnp.concatenate(
                    [ref[edge, :, lanes].reshape(TILE, LANES)]
                    + [ref[start, :, lanes] for start in starts[tile]],
                    axis=0,
                )

            mixed, total, top = attend(
                tile, lanes, gathered(keys), gathered(values), bias_far[tile]
            )
            near_top = max_near[rows, lanes]
            highest = jnp.maximum(near_top, top)
            near_part = jnp.exp(near_top - highest)
            far_part = jnp.exp(top - highest)
            mixed = acc_near[rows, lanes] * near_part + mixed * far_part
            total = sum_near[rows, lanes] * near_part + total * far_part
            out_ref[rows, lanes] = (mixed / total).astype(BF16)

    for copy in own + far + edges:
        copy.wait_send()


def local(
    features,
    query_weight,
    key_weight,
    value_weight,
    out_weight,
    band_reach,
    long_peers,
    long_count,
    send_tile,
):
    hbm = pl.BlockSpec(memory_space=pltpu.HBM)
    flows = len(X_ORDER) + 1
    dma = pltpu.SemaphoreType.DMA
    attended = pl.pallas_call(
        kernel,
        name="layer",
        out_shape=pltpu.VMEM((ROWS, D), BF16),
        in_specs=[pl.BlockSpec(memory_space=pltpu.SMEM)] + [hbm] * 7,
        out_specs=pl.BlockSpec(memory_space=pltpu.VMEM),
        scratch_shapes=[
            pltpu.SMEM((2, MAXLONG), jnp.int32),
            pltpu.SMEM((2,), jnp.int32),
            pltpu.SMEM((1, 16), jnp.int32),
            pltpu.VMEM((ROWS, D), BF16),
            pltpu.VMEM((D, D), BF16),
            pltpu.VMEM((D, D), BF16),
            pltpu.VMEM((D, D), BF16),
            pltpu.VMEM((4, PORTAL, D), BF16),
            pltpu.VMEM((4, PORTAL, D), BF16),
            pltpu.SMEM((1, 16), jnp.int32),
            pltpu.VMEM((SLOTS + 4, PORTAL, D), BF16),
            pltpu.VMEM((flows, PORTAL, D), BF16),
            pltpu.VMEM((flows, PORTAL, D), BF16),
            pltpu.VMEM((4, PORTAL, D), BF16),
            pltpu.VMEM((HALO + 4, PORTAL, D), BF16),
            pltpu.VMEM((HALO + 4, PORTAL, D), BF16),
            pltpu.VMEM((ROWS, ROWS), F32),
            pltpu.VMEM((2, TILE, TILE + MAXLONG * PORTAL), F32),
            pltpu.VMEM((ROWS, D), F32),
            pltpu.VMEM((ROWS, D), F32),
            pltpu.VMEM((ROWS, D), F32),
            dma((7,)),
            dma((flows,)),
            dma((flows,)),
            dma((flows,)),
            dma((flows,)),
            dma((2,)),
            dma((2,)),
            dma((2,)),
            dma((2,)),
            pltpu.SemaphoreType.REGULAR((2,)),
        ],
        compiler_params=pltpu.CompilerParams(
            collective_id=0, has_side_effects=True, vmem_limit_bytes=50 * 1024 * 1024
        ),
    )(
        band_reach,
        *(
            pltpu.with_memory_space_constraint(operand, pltpu.HBM)
            for operand in (
                long_peers,
                long_count,
                send_tile,
                features,
                query_weight,
                key_weight,
                value_weight,
            )
        )
    )
    projected = jnp.dot(attended, out_weight, preferred_element_type=F32)
    return (features.astype(F32) + projected).astype(BF16)


def solution(mesh):
    return jax.shard_map(
        local,
        mesh=mesh,
        in_specs=(
            P(("grp", "rng"), None),
            P(),
            P(),
            P(),
            P(),
            P(("grp", "rng")),
            P(("grp", "rng"), None),
            P(("grp", "rng")),
            P(("grp", "rng"), None),
        ),
        out_specs=P(("grp", "rng"), None),
        check_vma=False,
    )
```

```python
import functools

import jax
import jax.numpy as jnp
from jax import lax
from jax.experimental import pallas as pl
from jax.experimental.pallas import tpu as pltpu
from jax.sharding import PartitionSpec as P

MESH = pl.DeviceIdType.MESH
F32 = jnp.float32
BF16 = jnp.bfloat16

EPSILON = 1e-06
D = 1024
ROWS = 256
TILE = 128
PORTAL = 64
MAXLONG = 6
LANES = 128
PAIRS = D // LANES
SCALE = 64 ** (-0.5)
FLOOR = -3.0e38

GRAY = {0: 0, 1: 1, 2: 3, 3: 2}
X_ORDER = ((1, 0), (3, 0), (1, 1), (3, 1), (2, 0), (2, 1))
NEAR_BLOCKS = 4
SLOTS = 16
HALO = NEAR_BLOCKS + SLOTS


def project(src, block, count, pairs, dst_block, scale=None):
    rows = count * PORTAL
    width = D // 2

    @pl.loop(0, 2, unroll=True)
    def _(step):
        columns = pl.ds(pl.multiple_of(step * width, width), width)
        for weight, dst in pairs:
            total = jnp.dot(
                src[pl.ds(block, count)].reshape(rows, D),
                weight[:, columns],
                preferred_element_type=F32,
            ).astype(BF16)
            if scale is not None:
                total = total * jnp.asarray(scale, BF16)
            dst[pl.ds(dst_block, count), :, columns] = total.reshape(count, PORTAL, width)


def kernel(
    reach_ref,
    peers_hbm,
    count_hbm,
    pick_hbm,
    feat_hbm,
    wq_hbm,
    wk_hbm,
    wv_hbm,
    out_ref,
    peers_ref,
    count_ref,
    pick_ref,
    feat,
    wq,
    wk,
    wv,
    normed,
    partner,
    partner_pick,
    arrived,
    stage_own,
    stage_far,
    queries,
    keys,
    values,
    bias_near,
    bias_far,
    acc_near,
    sum_near,
    max_near,
    in_sem,
    send_own,
    recv_own,
    send_far,
    recv_far,
    send_y,
    recv_y,
    send_halo,
    recv_halo,
    ready,
):
    g = lax.axis_index("grp")
    r = lax.axis_index("rng")
    x, row_bit, core = g // 4, (g // 2) % 2, g % 2

    def device(dx, dy, dc):
        return (
            lax.rem(x + dx, 4) * 4 + lax.rem(row_bit + dy, 2) * 2 + lax.rem(core + dc, 2),
            r,
        )

    above = (g, lax.rem(r + 1, 16))
    below = (g, lax.rem(r + 15, 16))
    row_flows = X_ORDER + ((0, 1),)

    def loads_of(first, *pairs):
        return [
            pltpu.make_async_copy(src, dst, in_sem.at[first + i])
            for i, (src, dst) in enumerate(pairs)
        ]

    feat_load, pick_load, *small_loads = loads_of(
        0,
        (feat_hbm, feat),
        (pick_hbm, pick_ref),
        (peers_hbm, peers_ref),
        (count_hbm, count_ref),
    )
    loads = loads_of(4, (wq_hbm, wq), (wk_hbm, wk), (wv_hbm, wv))
    for load in (feat_load, pick_load, *small_loads):
        load.start()

    odd = lax.rem(r, 2)
    barrier = pltpu.get_barrier_semaphore()
    friends = [device(dx, 0, dc) for dx, dc in row_flows] + [device(0, 1, 0)]
    for friend in friends:
        pl.semaphore_signal(barrier, inc=1, device_id=friend, device_id_type=MESH)

    @pl.when(odd == 0)
    def _():
        for neighbour in (above, below):
            pl.semaphore_signal(barrier, inc=1, device_id=neighbour, device_id_type=MESH)

    feat_load.wait()
    for load in loads:
        load.start()

    @pl.loop(0, ROWS // PORTAL)
    def _(block):
        rows = pl.ds(pl.multiple_of(block * PORTAL, PORTAL), PORTAL)
        widened = feat[rows, :].astype(F32)
        factor = lax.rsqrt(jnp.mean(widened * widened, axis=1, keepdims=True) + EPSILON)
        normed[block] = (widened * factor).astype(BF16)

    def slot_of_flow(dx, dc, far):
        return 8 * far + 2 * GRAY[dx] + dc

    pick_load.wait()
    pl.semaphore_wait(barrier, len(friends) + 2 * odd)

    @pl.when(odd == 1)
    def _():
        for side, neighbour in enumerate((above, below)):
            pl.semaphore_signal(
                ready.at[side], inc=1, device_id=neighbour, device_id_type=MESH
            )

    cross = [
        pltpu.make_async_remote_copy(
            src_ref=normed, dst_ref=partner, send_sem=send_y.at[0], recv_sem=recv_y.at[0],
            device_id=device(0, 1, 0), device_id_type=MESH,
        ),
        pltpu.make_async_remote_copy(
            src_ref=pick_ref, dst_ref=partner_pick, send_sem=send_y.at[1], recv_sem=recv_y.at[1],
            device_id=device(0, 1, 0), device_id_type=MESH,
        ),
    ]
    for copy in cross:
        copy.start()
    own = []
    for flow, (dx, dc) in enumerate(row_flows):
        target, _ = device(dx, 0, dc)
        stage_own[flow] = normed[pick_ref[0, target]]
        copy = pltpu.make_async_remote_copy(
            src_ref=stage_own.at[flow],
            dst_ref=arrived.at[slot_of_flow(dx, dc, 0)],
            send_sem=send_own.at[flow],
            recv_sem=recv_own.at[flow],
            device_id=device(dx, 0, dc),
            device_id_type=MESH,
        )
        copy.start()
        own.append(copy)

    for load in small_loads:
        load.wait()
    reach = reach_ref[0]
    place_q = lax.broadcasted_iota(jnp.int32, (ROWS, ROWS), 0)
    place_k = lax.broadcasted_iota(jnp.int32, (ROWS, ROWS), 1)
    bias_near[...] = jnp.where(jnp.abs(place_q - place_k) <= reach, 0.0, -jnp.inf)
    tile_q = lax.broadcasted_iota(jnp.int32, (TILE, TILE), 0)
    tile_k = lax.broadcasted_iota(jnp.int32, (TILE, TILE), 1)
    slot_of = lax.broadcasted_iota(jnp.int32, (TILE, MAXLONG * PORTAL), 1) // PORTAL
    for tile in range(2):
        gap = (tile_q - tile_k if tile == 0 else tile_k - tile_q) + TILE
        bias_far[tile, :, :TILE] = jnp.where(gap <= reach, 0.0, -jnp.inf)
        bias_far[tile, :, TILE:] = jnp.where(slot_of < count_ref[tile], 0.0, -jnp.inf)

    loads[0].wait()
    project(normed, 0, 4, ((wq, queries),), 0, SCALE)
    loads[1].wait()
    loads[2].wait()
    project(normed, 0, 4, ((wk, keys), (wv, values)), 0)

    even = lax.broadcasted_iota(jnp.int32, (TILE, LANES), 1) < LANES // 2

    def attend(tile, lanes, key_rows, value_rows, bias):
        query = queries[pl.ds(tile * 2, 2), :, lanes].reshape(TILE, LANES)
        none = jnp.zeros_like(query)
        wide = jnp.concatenate([value_rows, jnp.ones_like(value_rows)], axis=1)
        parts = []
        for head in (jnp.where(even, query, none), jnp.where(even, none, query)):
            scores = lax.dot_general(
                head, key_rows, (((1,), (1,)), ((), ())), preferred_element_type=F32
            )
            scores = scores + bias
            highest = jnp.maximum(jnp.max(scores, axis=1, keepdims=True), FLOOR)
            weights = jnp.exp(scores - highest).astype(BF16)
            mixed = jnp.dot(weights, wide, preferred_element_type=F32)
            parts.append(
                (mixed[:, :LANES], mixed[:, LANES:], jnp.broadcast_to(highest, (TILE, LANES)))
            )
        return [jnp.where(even, first, second) for first, second in zip(*parts)]

    @pl.loop(0, PAIRS, unroll=2)
    def _(pair):
        lanes = pl.ds(pl.multiple_of(pair * LANES, LANES), LANES)
        near = pl.ds(0, NEAR_BLOCKS)
        key_rows = keys[near, :, lanes].reshape(ROWS, LANES)
        value_rows = values[near, :, lanes].reshape(ROWS, LANES)
        for tile in range(2):
            rows = pl.ds(tile * TILE, TILE)
            mixed, total, top = attend(tile, lanes, key_rows, value_rows, bias_near[rows, :])
            acc_near[rows, lanes] = mixed
            sum_near[rows, lanes] = total
            max_near[rows, lanes] = top

    for copy in cross:
        copy.wait()

    def far_rows(target):
        return partner[partner_pick[0, target]]

    far = []
    for flow, (dx, dc) in enumerate(row_flows):
        target, _ = device(dx, 0, dc)
        stage_far[flow] = far_rows(target)
        copy = pltpu.make_async_remote_copy(
            src_ref=stage_far.at[flow],
            dst_ref=arrived.at[slot_of_flow(dx, dc, 1)],
            send_sem=send_far.at[flow],
            recv_sem=recv_far.at[flow],
            device_id=device(dx, 0, dc),
            device_id_type=MESH,
        )
        copy.start()
        far.append(copy)
    edges = [
        pltpu.make_async_remote_copy(
            src_ref=normed.at[pl.ds(2, 2)], dst_ref=arrived.at[pl.ds(SLOTS, 2)],
            send_sem=send_halo.at[0], recv_sem=recv_halo.at[0],
            device_id=above, device_id_type=MESH,
        ),
        pltpu.make_async_remote_copy(
            src_ref=normed.at[pl.ds(0, 2)], dst_ref=arrived.at[pl.ds(SLOTS + 2, 2)],
            send_sem=send_halo.at[1], recv_sem=recv_halo.at[1],
            device_id=below, device_id_type=MESH,
        ),
    ]
    @pl.when(odd == 0)
    def _():
        for side in range(2):
            pl.semaphore_wait(ready.at[side], 1)

    @pl.when(r != 0)
    def _():
        for copy in edges:
            copy.start()

    arrived[8] = far_rows(g)

    def project_slots(first, count):
        project(arrived, first, count, ((wk, keys), (wv, values)), NEAR_BLOCKS + first)

    for copy in own:
        copy.wait_recv()
    project_slots(1, 7)
    @pl.when(r == 0)
    def _():
        for copy in edges:
            copy.start()

    for flow in (6, 0, 1, 2, 3):
        far[flow].wait_recv()
    project_slots(8, 6)
    for copy in (far[4], far[5], *edges):
        copy.wait_recv()
    project_slots(14, 6)

    def slot_start(tile, entry):
        peer = peers_ref[tile, entry]
        dx = lax.rem(x + 4 - lax.div(peer, 4), 4)
        place = dx + lax.div(dx, 2) * (1 - 2 * lax.rem(dx, 2))
        other = lax.rem(lax.div(peer, 2) + row_bit, 2)
        turn = lax.rem(peer + core, 2)
        return NEAR_BLOCKS + 8 * other + 2 * place + turn

    starts = [[slot_start(tile, entry) for entry in range(MAXLONG)] for tile in range(2)]

    @pl.loop(0, PAIRS, unroll=True)
    def _(pair):
        lanes = pl.ds(pl.multiple_of(pair * LANES, LANES), LANES)
        for tile in range(2):
            rows = pl.ds(tile * TILE, TILE)
            edge = pl.ds(HALO + 2 * tile, 2)

            def gathered(ref):
                return jnp.concatenate(
                    [ref[edge, :, lanes].reshape(TILE, LANES)]
                    + [ref[start, :, lanes] for start in starts[tile]],
                    axis=0,
                )

            mixed, total, top = attend(
                tile, lanes, gathered(keys), gathered(values), bias_far[tile]
            )
            near_top = max_near[rows, lanes]
            highest = jnp.maximum(near_top, top)
            near_part = jnp.exp(near_top - highest)
            far_part = jnp.exp(top - highest)
            mixed = acc_near[rows, lanes] * near_part + mixed * far_part
            total = sum_near[rows, lanes] * near_part + total * far_part
            out_ref[rows, lanes] = (mixed / total).astype(BF16)

    for copy in own + far + edges:
        copy.wait_send()


def local(
    features,
    query_weight,
    key_weight,
    value_weight,
    out_weight,
    band_reach,
    long_peers,
    long_count,
    send_tile,
):
    hbm = pl.BlockSpec(memory_space=pltpu.HBM)
    flows = len(X_ORDER) + 1
    dma = pltpu.SemaphoreType.DMA
    attended = pl.pallas_call(
        kernel,
        name="layer",
        out_shape=pltpu.VMEM((ROWS, D), BF16),
        in_specs=[pl.BlockSpec(memory_space=pltpu.SMEM)] + [hbm] * 7,
        out_specs=pl.BlockSpec(memory_space=pltpu.VMEM),
        scratch_shapes=[
            pltpu.SMEM((2, MAXLONG), jnp.int32),
            pltpu.SMEM((2,), jnp.int32),
            pltpu.SMEM((1, 16), jnp.int32),
            pltpu.VMEM((ROWS, D), BF16),
            pltpu.VMEM((D, D), BF16),
            pltpu.VMEM((D, D), BF16),
            pltpu.VMEM((D, D), BF16),
            pltpu.VMEM((4, PORTAL, D), BF16),
            pltpu.VMEM((4, PORTAL, D), BF16),
            pltpu.SMEM((1, 16), jnp.int32),
            pltpu.VMEM((SLOTS + 4, PORTAL, D), BF16),
            pltpu.VMEM((flows, PORTAL, D), BF16),
            pltpu.VMEM((flows, PORTAL, D), BF16),
            pltpu.VMEM((4, PORTAL, D), BF16),
            pltpu.VMEM((HALO + 4, PORTAL, D), BF16),
            pltpu.VMEM((HALO + 4, PORTAL, D), BF16),
            pltpu.VMEM((ROWS, ROWS), F32),
            pltpu.VMEM((2, TILE, TILE + MAXLONG * PORTAL), F32),
            pltpu.VMEM((ROWS, D), F32),
            pltpu.VMEM((ROWS, D), F32),
            pltpu.VMEM((ROWS, D), F32),
            dma((7,)),
            dma((flows,)),
            dma((flows,)),
            dma((flows,)),
            dma((flows,)),
            dma((2,)),
            dma((2,)),
            dma((2,)),
            dma((2,)),
            pltpu.SemaphoreType.REGULAR((2,)),
        ],
        compiler_params=pltpu.CompilerParams(
            collective_id=0, has_side_effects=True, vmem_limit_bytes=50 * 1024 * 1024
        ),
    )(
        band_reach,
        *(
            pltpu.with_memory_space_constraint(operand, pltpu.HBM)
            for operand in (
                long_peers,
                long_count,
                send_tile,
                features,
                query_weight,
                key_weight,
                value_weight,
            )
        )
    )
    projected = jnp.dot(attended, out_weight, preferred_element_type=F32)
    return (features.astype(F32) + projected).astype(BF16)


def solution(mesh):
    return jax.shard_map(
        local,
        mesh=mesh,
        in_specs=(
            P(("grp", "rng"), None),
            P(),
            P(),
            P(),
            P(),
            P(("grp", "rng")),
            P(("grp", "rng"), None),
            P(("grp", "rng")),
            P(("grp", "rng"), None),
        ),
        out_specs=P(("grp", "rng"), None),
        check_vma=False,
    )
```
